32 devices in a mesh: dp: 2 (over x), tp: 4 (over z), kvp: 4 (over y, core).
Axes of the slice: x: 2, y: 2, z: 4, core: 2. Of those that a mesh axis runs over, the one named last changes fastest.
Arguments:
- x_in: bfloat16 [32, 5120], P('dp'), parts along dimension 0
- ctx_len: int32 [32], P('dp'), parts along dimension 0
- g_attn: bfloat16 [5120], replicated
- g_mlp: bfloat16 [5120], replicated
- w_qkv: bfloat16 [5120, 6144], P(None, 'tp')
- w_o: bfloat16 [4096, 5120], P(('tp', 'kvp'))
- w_gate: bfloat16 [5120, 32768], P(None, ('tp', 'kvp'))
- w_up: bfloat16 [5120, 32768], P(None, ('tp', 'kvp'))
- w_down: bfloat16 [32768, 5120], P(('tp', 'kvp'))
- k_cache: bfloat16 [32, 1024, 8, 128], P('dp', 'kvp', 'tp'), parts along dimension 0
- v_cache: bfloat16 [32, 1024, 8, 128], P('dp', 'kvp', 'tp'), parts along dimension 0
Outputs:
- output 1: bfloat16 [32, 5120], P('dp'), parts along dimension 0
- output 2: bfloat16 [32, 1024, 8, 128], P('dp', 'kvp', 'tp'), parts along dimension 0
- output 3: bfloat16 [32, 1024, 8, 128], P('dp', 'kvp', 'tp'), parts along dimension 0
There are 2 independent parts. The reference program is written for one: setup_inputs(seed, part) draws one part's arguments, and reference() takes and returns one part's arrays. A program takes and returns all parts, laid end to end along the dimension named above; an argument that names none is the same for every part.
All inputs are finite; a program needn't handle non-finite values.
Results may differ from the reference program's by a relative error of at most 0.00832932.
Values sent between devices are 32-bit elements.
A program may use at most 1 GiB of HBM per device.

```python
import jax
import jax.numpy as jnp
from jax import lax

D = 5120
HEADS = 32
KV_HEADS = 8
HEAD = 128
FF = 32768
BATCH = 16
SEQ = 1024
NSEG = 16
GROUP = HEADS // KV_HEADS
ROPE_THETA = 500000.0
EPS = 1e-5
NEG_FILL = -1e30


def rms_norm(values, gain_vec):
    x_f32 = values.astype(jnp.float32)
    inv_rms = lax.rsqrt(jnp.mean(x_f32 * x_f32, axis=-1, keepdims=True) + EPS)
    return (x_f32 * inv_rms * gain_vec.astype(jnp.float32)).astype(jnp.bfloat16)


def rope_tables(ctx_len):
    inv_freq = ROPE_THETA ** (-2.0 * jnp.arange(HEAD // 2, dtype=jnp.float32) / HEAD)
    angles = ctx_len.astype(jnp.float32)[:, None] * inv_freq[None, :]
    return jnp.cos(angles), jnp.sin(angles)


def rotary(vectors, cos_t, sin_t):
    half_dim = vectors.shape[-1] // 2
    first_half = vectors[..., :half_dim]
    second_half = vectors[..., half_dim:]
    return jnp.concatenate([first_half * cos_t - second_half * sin_t, second_half * cos_t + first_half * sin_t], axis=-1)


def setup_inputs(seed: int = 0, part: int = 0) -> dict:
    root_key = jax.random.key(seed)
    shared_keys = jax.random.split(root_key, 7)
    part_keys = jax.random.split(jax.random.fold_in(root_key, part), 7)
    x_in = jax.random.normal(part_keys[0], (BATCH, D), jnp.float32).astype(jnp.bfloat16)
    ctx_len = jax.random.randint(part_keys[1], (BATCH,), SEQ // 4, SEQ, dtype=jnp.int32)
    full_row = jax.random.randint(part_keys[2], (), 0, BATCH, dtype=jnp.int32)
    ctx_len = jnp.where(jnp.arange(BATCH) == full_row, SEQ - 1, ctx_len).astype(jnp.int32)
    g_attn = (1.0 + 0.3 * jax.random.normal(shared_keys[0], (D,), jnp.float32)).astype(jnp.bfloat16)
    g_mlp = (1.0 + 0.3 * jax.random.normal(shared_keys[1], (D,), jnp.float32)).astype(jnp.bfloat16)
    w_qkv = (jax.random.normal(shared_keys[2], (D, KV_HEADS * (GROUP + 2) * HEAD), jnp.float32) * D ** -0.5).astype(jnp.bfloat16)
    w_o = (jax.random.normal(shared_keys[3], (HEADS * HEAD, D), jnp.float32) * (HEADS * HEAD) ** -0.5).astype(jnp.bfloat16)
    w_gate = (jax.random.normal(shared_keys[4], (D, FF), jnp.float32) * D ** -0.5).astype(jnp.bfloat16)
    w_up = (jax.random.normal(shared_keys[5], (D, FF), jnp.float32) * D ** -0.5).astype(jnp.bfloat16)
    w_down = (jax.random.normal(shared_keys[6], (FF, D), jnp.float32) * FF ** -0.5).astype(jnp.bfloat16)
    seg_shape = (BATCH, NSEG, 1, KV_HEADS, HEAD)
    noise_shape = (BATCH, NSEG, SEQ // NSEG, KV_HEADS, HEAD)
    cache_shape = (BATCH, SEQ, KV_HEADS, HEAD)
    k_cache = (jax.random.normal(part_keys[3], noise_shape, jnp.float32) + 0.5 * jax.random.normal(part_keys[4], seg_shape, jnp.float32)).reshape(cache_shape).astype(jnp.bfloat16)
    v_cache = (0.5 * jax.random.normal(part_keys[5], noise_shape, jnp.float32) + 2.0 * jax.random.normal(part_keys[6], seg_shape, jnp.float32)).reshape(cache_shape).astype(jnp.bfloat16)
    return {"x_in": x_in, "ctx_len": ctx_len, "g_attn": g_attn, "g_mlp": g_mlp, "w_qkv": w_qkv, "w_o": w_o, "w_gate": w_gate, "w_up": w_up, "w_down": w_down, "k_cache": k_cache, "v_cache": v_cache}


def reference(x_in, ctx_len, g_attn, g_mlp, w_qkv, w_o, w_gate, w_up, w_down, k_cache, v_cache):
    normed = rms_norm(x_in, g_attn)
    qkv_all = jnp.dot(normed, w_qkv, preferred_element_type=jnp.float32).reshape(BATCH, KV_HEADS, GROUP + 2, HEAD)
    cos_t, sin_t = rope_tables(ctx_len)
    queries = rotary(qkv_all[:, :, :GROUP], cos_t[:, None, None, :], sin_t[:, None, None, :]).astype(jnp.bfloat16)
    key_new = rotary(qkv_all[:, :, GROUP], cos_t[:, None, :], sin_t[:, None, :]).astype(jnp.bfloat16)
    val_new = qkv_all[:, :, GROUP + 1].astype(jnp.bfloat16)
    positions = jnp.arange(SEQ)
    hit_mask = (positions[None, :] == ctx_len[:, None])[:, :, None, None]
    k_out = jnp.where(hit_mask, key_new[:, None], k_cache)
    v_out = jnp.where(hit_mask, val_new[:, None], v_cache)
    score_scale = HEAD ** -0.5

    def one_request(row_args):
        q_row, k_row, v_row, length = row_args
        scores = jnp.einsum("grd,tgd->grt", q_row.astype(jnp.float32), k_row.astype(jnp.float32)) * score_scale
        scores = jnp.where(positions <= length, scores, NEG_FILL)
        row_max = jnp.max(scores, axis=-1, keepdims=True)
        prob_w = jnp.exp(scores - row_max)
        denom_sum = jnp.sum(prob_w, axis=-1)
        numer_acc = jnp.einsum("grt,tgd->grd", prob_w.astype(jnp.bfloat16).astype(jnp.float32), v_row.astype(jnp.float32))
        return (numer_acc / denom_sum[..., None]).reshape(HEADS * HEAD)

    attn_all = lax.map(one_request, (queries, k_out, v_out, ctx_len)).astype(jnp.bfloat16)
    hidden = (x_in.astype(jnp.float32) + jnp.dot(attn_all, w_o, preferred_element_type=jnp.float32)).astype(jnp.bfloat16)
    normed_mlp = rms_norm(hidden, g_mlp)
    gate_pre = jnp.dot(normed_mlp, w_gate, preferred_element_type=jnp.float32)
    up_proj = jnp.dot(normed_mlp, w_up, preferred_element_type=jnp.float32)
    act_out = (jax.nn.silu(gate_pre) * up_proj).astype(jnp.bfloat16)
    x_out = (hidden.astype(jnp.float32) + jnp.dot(act_out, w_down, preferred_element_type=jnp.float32)).astype(jnp.bfloat16)
    return (x_out, k_out, v_out)
```

```python
import functools

import jax
import jax.numpy as jnp
import numpy as np
from jax import lax
from jax.experimental import pallas as pl
from jax.experimental.pallas import tpu as pltpu
from jax.sharding import PartitionSpec as P

ROPE_THETA = 500000.0
EPS = 1e-5
NEG_FILL = -1e30
MESH = pl.DeviceIdType.MESH
BF = jnp.bfloat16
F32 = jnp.float32
LANES = 128
TILE = 256
VMEM_BYTES = 67_043_328


def _layer_kernel(dims, ctx_ref, x_hbm, ga_hbm, gm_hbm, freq_hbm, wqkv_hbm, wo_hbm, wg_hbm, wu_hbm, wd_hbm, k_hbm, v_hbm,
                  out_ref, new_ref,
                  w, xb, ga, gm, freq, xf, nrm, qkv, qs, kn, vn, sc, pr, accx, mlx, racc, rml, part, recv_a, recv_b, full, act,
                  sem_in, sem_qkv, sem_kv, sem_wo, sem_gu, sem_dn, s_x, r_x, s_a, r_a, s_b, r_b, s_c, r_c, s_d, r_d):
    batch, width, ff, kv_loc, group, head, block_len, n_tp, n_kvp = dims
    half = batch // 2
    chips = n_tp * n_kvp // 2
    piece = width // chips
    heads = kv_loc * group
    n_qkv = kv_loc * (group + 2) * head // TILE
    n_gu = ff // TILE
    n_dn = width // TILE
    rows_o = wo_hbm.shape[0]
    cols = kv_loc * block_len

    up0 = n_gu * width
    dn0 = 2 * n_gu * width
    kv0 = dn0 - 2 * width
    wo0 = dn0 + n_qkv * width

    tp = lax.axis_index("tp")
    kvp = lax.axis_index("kvp")
    core = kvp % 2
    y = kvp // 2
    me = tp * 2 + y
    pal = kvp + 1 - 2 * core

    def flip(bits):
        hi, lo = bits // 2, bits % 2
        z = tp
        if hi == 3:
            z = 3 - tp
        elif hi == 2:
            z = (tp + 2) % 4
        elif hi == 1:
            z = tp + 1 - 2 * (tp % 2)
        yy = 1 - y if lo else y
        return z, yy

    peers = [flip(b) for b in (7, 5, 3, 6, 4, 2, 1)]

    def at(z, k):
        return {"tp": z, "kvp": k}

    small = [pltpu.make_async_copy(s, d, sem_in.at[i]) for i, (s, d) in enumerate(((x_hbm, xb), (ga_hbm, ga), (freq_hbm, freq), (gm_hbm, gm)))]

    def qkv_copy(n):
        return pltpu.make_async_copy(wqkv_hbm.at[:, pl.ds(n * TILE, TILE)], w.at[pl.ds(dn0 + n * width, width), :], sem_qkv.at[n])

    def wo_copy(n):
        return pltpu.make_async_copy(wo_hbm.at[:, pl.ds(n * TILE, TILE)], w.at[pl.ds(wo0 + n * rows_o, rows_o), :], sem_wo)

    def gate_copy(j):
        return pltpu.make_async_copy(wg_hbm.at[:, pl.ds(j * TILE, TILE)], w.at[pl.ds(j * width, width), :], sem_gu.at[2 * j])

    def up_copy(j):
        return pltpu.make_async_copy(wu_hbm.at[:, pl.ds(j * TILE, TILE)], w.at[pl.ds(up0 + j * width, width), :], sem_gu.at[2 * j + 1])

    def dn_copy(n):
        return pltpu.make_async_copy(wd_hbm.at[:, pl.ds(n * TILE, TILE)], w.at[pl.ds(dn0 + n * ff, ff), :], sem_dn.at[n])

    k_copy = pltpu.make_async_copy(k_hbm, w.at[pl.ds(kv0, batch * cols), pl.ds(0, head)], sem_kv.at[0])
    v_copy = pltpu.make_async_copy(v_hbm, w.at[pl.ds(kv0, batch * cols), pl.ds(head, head)], sem_kv.at[1])

    for c in small:
        c.start()
    for n in range(n_qkv):
        qkv_copy(n).start()
    k_copy.start()
    v_copy.start()
    for n in range(n_dn):
        wo_copy(n).start()
    for j in range(n_gu - 2):
        gate_copy(j).start()
        up_copy(j).start()

    barrier = pltpu.get_barrier_semaphore()
    greet = [at(z, yy * 2 + core) for z, yy in peers] + [at(tp, pal), at(tp, (1 - y) * 2 + 1 - core)]
    for d in greet:
        pl.semaphore_signal(barrier, inc=1, device_id=d, device_id_type=MESH)

    for c in small:
        c.wait()
    xv = xb[...].astype(F32)
    inv = lax.rsqrt(jnp.mean(xv * xv, axis=-1, keepdims=True) + EPS)
    nrm[...] = (xv * inv * ga[...].reshape(1, width).astype(F32)).astype(BF)
    for r in range(2):
        xf[r] = xv[r * half:(r + 1) * half]

    rows_i = lax.broadcasted_iota(jnp.int32, (batch, head), 0)
    pos = jnp.zeros((batch, head), F32)
    for b in range(batch):
        pos = jnp.where(rows_i == b, ctx_ref[b].astype(F32), pos)
    angle = pos * freq[0:1, :]
    lane = lax.broadcasted_iota(jnp.int32, (batch, head), 1)
    cos_t = jnp.cos(angle)
    sin_t = jnp.sin(angle)
    sin_t = jnp.where(lane < head // 2, -sin_t, sin_t)

    def qkv_step(i, carry):
        for u in range(2):
            qkv_copy(2 * i + u).wait()
        for u in range(2):
            n = 2 * i + u
            qkv[n] = jnp.dot(nrm[...], w[pl.ds(dn0 + n * width, width), :], preferred_element_type=F32)
        return carry

    lax.fori_loop(0, n_qkv // 2, qkv_step, 0)

    def column(j):
        return qkv[j // 2, :, (j % 2) * head:(j % 2 + 1) * head]

    def rotary(v):
        return (v * cos_t + pltpu.roll(v, head // 2, 1) * sin_t).astype(BF).astype(F32)

    for g in range(kv_loc):
        base = g * (group + 2)
        for r in range(group):
            qs[pl.ds(g * group + r, batch, stride=heads), :] = rotary(column(base + r))
        key = rotary(column(base + group))
        val = column(base + group + 1).astype(BF).astype(F32)
        new_ref[g] = key
        new_ref[kv_loc + g] = val
        for r in range(group):
            kn[pl.ds(g * group + r, batch, stride=heads), :] = key
            vn[pl.ds(g * group + r, batch, stride=heads), :] = val

    k_copy.wait()
    v_copy.wait()
    scale = head ** -0.5
    for b in range(batch):
        q_b = qs[b * heads:(b + 1) * heads, :].astype(BF)
        k_b = w[pl.ds(kv0 + b * cols, cols), 0:head]
        sc[b] = lax.dot_general(q_b, k_b, (((1,), (1,)), ((), ())), preferred_element_type=F32)
    s_new = jnp.sum(qs[...] * kn[...], axis=-1, keepdims=True) * scale
    col_i = lax.broadcasted_iota(jnp.int32, (heads, cols), 1)
    row_i = lax.broadcasted_iota(jnp.int32, (heads, cols), 0)
    own = (col_i % kv_loc) == (row_i // group)
    t_i = col_i // kv_loc
    lane_h = lax.broadcasted_iota(jnp.int32, (heads, head), 1)
    p_new = []
    for b in range(batch):
        here = ctx_ref[b] - kvp * block_len
        fresh = s_new[b * heads:(b + 1) * heads]
        is_new = own & (t_i == here)
        s = jnp.where(is_new, fresh, sc[b] * scale)
        s = jnp.where(own & (t_i <= here), s, NEG_FILL)
        m = jnp.max(s, axis=-1, keepdims=True)
        p = jnp.exp(s - m)
        total = jnp.sum(p, axis=-1, keepdims=True)
        p_new.append(jnp.max(jnp.where(is_new, p, 0.0), axis=-1, keepdims=True).astype(BF).astype(F32))
        pr[b] = jnp.where(is_new, 0.0, p).astype(BF)
        mlx[pl.ds(b, heads, stride=batch), :] = jnp.where(lane_h < head // 2, m, total)
    for b in range(batch):
        v_b = w[pl.ds(kv0 + b * cols, cols), head:2 * head]
        o = jnp.dot(pr[b], v_b, preferred_element_type=F32)
        accx[pl.ds(b, heads, stride=batch), :] = o + p_new[b] * vn[b * heads:(b + 1) * heads, :]

    for j in range(n_gu - 2, n_gu):
        gate_copy(j).start()
        up_copy(j).start()
    late = [n for n in range(n_dn) if dn0 + (n + 1) * ff > wo0 and dn0 + n * ff < wo0 + n_dn * rows_o]
    for n in range(n_dn):
        if n not in late:
            dn_copy(n).start()

    pl.semaphore_wait(barrier, len(greet))
    rows = heads // n_kvp * batch
    sent = []
    for d in (3, 2, 1):
        to = (kvp + d) % n_kvp
        frm = (kvp + n_kvp - d) % n_kvp
        for i, (src, dst) in enumerate(((accx, racc), (mlx, rml))):
            c = pltpu.make_async_remote_copy(src.at[pl.ds(to * rows, rows), :], dst.at[kvp], s_x.at[2 * d - 2 + i], r_x.at[2 * d - 2 + i],
                                             device_id=at(tp, to), device_id_type=MESH)
            c.start()
            sent.append(c)
    mine = pl.ds(pl.multiple_of(kvp * rows, rows), rows)
    racc[kvp] = accx[mine, :]
    rml[kvp] = mlx[mine, :]
    for c in sent:
        c.wait()
    ml = [rml[i] for i in range(n_kvp)]
    top = functools.reduce(jnp.maximum, ml)
    wt = [jnp.exp(v[:, 0:1] - top[:, 0:1]) for v in ml]
    den = sum(a * v[:, head // 2:head // 2 + 1] for a, v in zip(wt, ml))
    num = sum(a * racc[i] for i, a in enumerate(wt))
    a_f = num / den
    a_own = jnp.concatenate([a_f[r * batch:(r + 1) * batch] for r in range(rows // batch)], axis=1).astype(BF)

    for n in range(n_dn):
        wo_copy(n).wait()
    for n in range(n_dn):
        r = jnp.dot(a_own, w[pl.ds(wo0 + n * rows_o, rows_o), :], preferred_element_type=F32)
        part[0, :, n * TILE:(n + 1) * TILE] = r[:half]
        part[1, :, n * TILE:(n + 1) * TILE] = r[half:]
    for n in late:
        dn_copy(n).start()

    def span(chip):
        return pl.ds(pl.multiple_of(chip * piece, LANES), piece)

    def all_reduce(step, finish):
        sends = []
        a = pltpu.make_async_remote_copy(part.at[1 - core], recv_a.at[step], s_a.at[step], r_a.at[step], device_id=at(tp, pal), device_id_type=MESH)
        a.start()
        a.wait_recv()
        part[core] = part[core] + recv_a[step]
        for i, (z, yy) in enumerate(peers):
            c = pltpu.make_async_remote_copy(part.at[core, :, span(z * 2 + yy)], recv_b.at[step, i], s_b.at[step, i], r_b.at[step, i],
                                             device_id=at(z, yy * 2 + core), device_id_type=MESH)
            c.start()
            sends.append(c)
        total = part[core, :, span(me)]
        for i in range(len(peers)):
            sends[i].wait_recv()
            total = total + recv_b[step, i]
        full[step, core, :, span(me)] = finish(total)
        outs, fwd = [], []
        own_view = full.at[step, core, :, span(me)]
        for i, (z, yy) in enumerate(peers):
            c = pltpu.make_async_remote_copy(own_view, own_view, s_c.at[step, i], r_c.at[step, i], device_id=at(z, yy * 2 + core), device_id_type=MESH)
            c.start()
            outs.append(c)

        def forward(i, chip):
            view = full.at[step, core, :, span(chip)]
            c = pltpu.make_async_remote_copy(view, view, s_d.at[step, i], r_d.at[step, i], device_id=at(tp, pal), device_id_type=MESH)
            c.start()
            fwd.append(c)

        forward(len(peers), me)
        for i in reversed(range(len(peers))):
            outs[i].wait_recv()
            forward(i, peers[i][0] * 2 + peers[i][1])
        for c in fwd:
            c.wait_recv()
        a.wait_send()
        for c in sends + outs + fwd:
            c.wait_send()

    def finish_attention(total):
        return (xf[core, :, span(me)] + total).astype(BF).astype(F32)

    all_reduce(0, finish_attention)

    gain = gm[...].reshape(1, width).astype(F32)
    hv = jnp.concatenate([full[0, 0], full[0, 1]], axis=0)
    inv2 = lax.rsqrt(jnp.mean(hv * hv, axis=-1, keepdims=True) + EPS)
    nrm[...] = (hv * inv2 * gain).astype(BF)

    def gu_step(j, carry):
        gate_copy(j).wait()
        up_copy(j).wait()
        g_v = jnp.dot(nrm[...], w[pl.ds(j * width, width), :], preferred_element_type=F32)
        u_v = jnp.dot(nrm[...], w[pl.ds(up0 + j * width, width), :], preferred_element_type=F32)
        act[j] = (jax.nn.silu(g_v) * u_v).astype(BF)
        return carry

    lax.fori_loop(0, n_gu, gu_step, 0)
    av = jnp.concatenate([act[j] for j in range(n_gu)], axis=1)

    def dn_step(i, carry):
        for u in range(2):
            dn_copy(2 * i + u).wait()
        for u in range(2):
            n = 2 * i + u
            r = jnp.dot(av, w[pl.ds(dn0 + n * ff, ff), :], preferred_element_type=F32)
            sl = pl.ds(pl.multiple_of(n * TILE, TILE), TILE)
            part[0, :, sl] = r[:half]
            part[1, :, sl] = r[half:]
        return carry

    lax.fori_loop(0, n_dn // 2, dn_step, 0)

    def finish_mlp(total):
        return (full[0, core, :, span(me)] + total).astype(BF).astype(F32)

    all_reduce(1, finish_mlp)
    out_ref[...] = jnp.concatenate([full[1, 0], full[1, 1]], axis=0).astype(BF)


def _cache_kernel(dims, ctx_ref, new_ref, k_hbm, v_hbm, ko_hbm, vo_hbm, kbuf, vbuf, sem_i, sem_o):
    batch, block_len, kv_loc, chunks = dims
    kvp = lax.axis_index("kvp")
    size = batch // chunks
    jobs = [(i, c) for c in range(chunks) for i in range(2)]

    def load(i, c):
        src, buf = ((k_hbm, kbuf), (v_hbm, vbuf))[i]
        sl = pl.ds(c * size, size)
        return pltpu.make_async_copy(src.at[sl], buf.at[sl], sem_i.at[i, c])

    def save(i, c):
        dst, buf = ((ko_hbm, kbuf), (vo_hbm, vbuf))[i]
        sl = pl.ds(c * size, size)
        return pltpu.make_async_copy(buf.at[sl], dst.at[sl], sem_o.at[i, c])

    for j in jobs:
        load(*j).start()
    for i, c in jobs:
        load(i, c).wait()
        buf = (kbuf, vbuf)[i]
        for b in range(c * size, (c + 1) * size):
            here = ctx_ref[b] - kvp * block_len

            @pl.when((here >= 0) & (here < block_len))
            def _():
                rows = [new_ref[i * kv_loc + g, b:b + 1, :] for g in range(kv_loc)]
                buf[b, jnp.clip(here, 0, block_len - 1)] = jnp.concatenate(rows, axis=0).astype(BF)

        save(i, c).start()
    for j in jobs:
        save(*j).wait()


def solution(mesh):
    n_tp, n_kvp = mesh.shape["tp"], mesh.shape["kvp"]
    x_spec = P("dp", None)
    cache_spec = P("dp", "kvp", "tp", None)
    model_axes = ("tp", "kvp")

    def layer_step(x_in, ctx_len, g_attn, g_mlp, w_qkv, w_o, w_gate, w_up, w_down, k_cache, v_cache):
        batch, block_len, kv_loc, head = k_cache.shape
        width = x_in.shape[1]
        ff = w_gate.shape[1]
        group = w_qkv.shape[1] // (kv_loc * head) - 2
        heads = kv_loc * group
        chips = n_tp * n_kvp // 2
        n_qkv, n_gu, n_dn = w_qkv.shape[1] // TILE, ff // TILE, width // TILE
        half = batch // 2
        rows = heads // n_kvp * batch
        freq = (ROPE_THETA ** (-2.0 * np.arange(head // 2) / head)).astype(np.float32)
        freq = jnp.asarray(np.tile(np.concatenate([freq, freq])[None], (8, 1)))
        flat = (batch * block_len * kv_loc, head)
        hbm = pl.BlockSpec(memory_space=pl.ANY)
        smem = pl.BlockSpec(memory_space=pltpu.SMEM)
        vmem = pl.BlockSpec(memory_space=pltpu.VMEM)
        dma = pltpu.SemaphoreType.DMA
        peers = chips - 1
        dims = (batch, width, ff, kv_loc, group, head, block_len, n_tp, n_kvp)
        x_out, new = pl.pallas_call(
            functools.partial(_layer_kernel, dims),
            out_shape=(jax.ShapeDtypeStruct((batch, width), BF), jax.ShapeDtypeStruct((2 * kv_loc, batch, head), F32)),
            in_specs=[smem] + [hbm] * 11,
            out_specs=(vmem, vmem),
            scratch_shapes=[
                pltpu.VMEM((3 * ff * width // TILE, TILE), BF),
                pltpu.VMEM((batch, width), BF),
                pltpu.VMEM((width,), BF),
                pltpu.VMEM((width,), BF),
                pltpu.VMEM((8, head), F32),
                pltpu.VMEM((2, half, width), F32),
                pltpu.VMEM((batch, width), BF),
                pltpu.VMEM((n_qkv, batch, TILE), F32),
                pltpu.VMEM((batch * heads, head), F32),
                pltpu.VMEM((batch * heads, head), F32),
                pltpu.VMEM((batch * heads, head), F32),
                pltpu.VMEM((batch, heads, kv_loc * block_len), F32),
                pltpu.VMEM((batch, heads, kv_loc * block_len), BF),
                pltpu.VMEM((batch * heads, head), F32),
                pltpu.VMEM((batch * heads, head), F32),
                pltpu.VMEM((n_kvp, rows, head), F32),
                pltpu.VMEM((n_kvp, rows, head), F32),
                pltpu.VMEM((2, half, width), F32),
                pltpu.VMEM((2, half, width), F32),
                pltpu.VMEM((2, peers, half, width // chips), F32),
                pltpu.VMEM((2, 2, half, width), F32),
                pltpu.VMEM((n_gu, batch, TILE), BF),
                dma((4,)), dma((n_qkv,)), dma((2,)), dma, dma((2 * n_gu,)), dma((n_dn,)),
                dma((6,)), dma((6,)), dma((2,)), dma((2,)),
                dma((2, peers)), dma((2, peers)), dma((2, peers)), dma((2, peers)), dma((2, peers + 1)), dma((2, peers + 1)),
            ],
            compiler_params=pltpu.CompilerParams(collective_id=0, has_side_effects=True, vmem_limit_bytes=VMEM_BYTES),
            name="layer",
        )(ctx_len, x_in, g_attn, g_mlp, freq, w_qkv, w_o, w_gate, w_up, w_down, k_cache.reshape(flat), v_cache.reshape(flat))
        chunks = 4
        k_out, v_out = pl.pallas_call(
            functools.partial(_cache_kernel, (batch, block_len, kv_loc, chunks)),
            out_shape=(jax.ShapeDtypeStruct(k_cache.shape, BF), jax.ShapeDtypeStruct(v_cache.shape, BF)),
            in_specs=[smem, vmem, hbm, hbm],
            out_specs=(hbm, hbm),
            scratch_shapes=[pltpu.VMEM(k_cache.shape, BF), pltpu.VMEM(v_cache.shape, BF), dma((2, chunks)), dma((2, chunks))],
            compiler_params=pltpu.CompilerParams(vmem_limit_bytes=VMEM_BYTES),
            name="cache",
        )(ctx_len, new, k_cache, v_cache)
        return x_out, k_out, v_out

    in_specs = (x_spec, P("dp"), P(None), P(None), P(None, "tp"), P(model_axes, None), P(None, model_axes), P(None, model_axes), P(model_axes, None), cache_spec, cache_spec)
    return jax.shard_map(layer_step, mesh=mesh, in_specs=in_specs, out_specs=(x_spec, cache_spec, cache_spec), check_vma=False)
```

```python
import functools

import jax
import jax.numpy as jnp
import numpy as np
from jax import lax
from jax.experimental import pallas as pl
from jax.experimental.pallas import tpu as pltpu
from jax.sharding import PartitionSpec as P

ROPE_THETA = 500000.0
EPS = 1e-5
NEG_FILL = -1e30
MESH = pl.DeviceIdType.MESH
BF = jnp.bfloat16
F32 = jnp.float32
LANES = 128
TILE = 256
VMEM_BYTES = 67_043_328


class _Phase:
    def __init__(self):
        self.scope = None

    def __call__(self, name):
        if self.scope is not None:
            self.scope.__exit__(None, None, None)
        self.scope = None
        if name:
            self.scope = jax.named_scope(name)
            self.scope.__enter__()


def _layer_kernel(dims, ctx_hbm, x_hbm, ga_hbm, gm_hbm, freq_hbm, wqkv_hbm, wo_hbm, wg_hbm, wu_hbm, wd_hbm, k_hbm, v_hbm,
                  out_ref, new_ref,
                  ctx_ref, wg, wu, wd, xb, ga, gm, freq, xf, nrm, gmx, qkv, qs, kn, vn, sc, pr, accx, mlx, racc, rml, part, recv_a, recv_b, full,
                  ssb, acc_g, acc_u, act,
                  sem_in, sem_qkv, sem_kv, sem_wo, sem_gu, sem_dn, s_q, r_q, s_x, r_x, s_s, r_s, s_a, r_a, s_b, r_b, s_c, r_c, s_d, r_d):
    batch, width, ff, kv_loc, group, head, block_len, n_tp, n_kvp = dims
    half = batch // 2
    chips = n_tp * n_kvp // 2
    piece = width // chips
    block = 2 * piece
    tiles = block // TILE
    heads = kv_loc * group
    n_qkv = kv_loc * (group + 2) * head // TILE
    q_loc = n_qkv // 2
    n_gu = ff // TILE
    n_dn = width // TILE
    rows_o = wo_hbm.shape[0]
    cols = kv_loc * block_len
    kv0 = q_loc * width
    wo0 = kv0 + batch * cols
    wo_end = wo0 + n_dn * rows_o

    phase = _Phase()
    phase("loads")
    tp = lax.axis_index("tp")
    kvp = lax.axis_index("kvp")
    core = kvp % 2
    y = kvp // 2
    me = tp * 2 + y
    pal = kvp + 1 - 2 * core
    zs = [tp, tp + 1 - 2 * (tp % 2), (tp + 2) % 4, 3 - tp]
    ys = [y, 1 - y]
    cores = [core, 1 - core]

    def device(e, lo, cc=0):
        return {"tp": zs[e], "kvp": ys[lo] * 2 + cores[cc]}

    def remote(src, dst, send, recv, to):
        return pltpu.make_async_remote_copy(src, dst, send, recv, device_id=to, device_id_type=MESH)

    def aligned(start, size):
        return pl.ds(pl.multiple_of(start, LANES), size)

    small = [pltpu.make_async_copy(s, d, sem_in.at[i]) for i, (s, d) in enumerate(((x_hbm, xb), (ga_hbm, ga), (freq_hbm, freq), (ctx_hbm, ctx_ref), (gm_hbm, gm)))]

    def qkv_copy(n):
        return pltpu.make_async_copy(wqkv_hbm.at[:, aligned((core * q_loc + n) * TILE, TILE)], wd.at[pl.ds(n * width, width), :], sem_qkv.at[n])

    def wo_copy(n):
        return pltpu.make_async_copy(wo_hbm.at[:, pl.ds(n * TILE, TILE)], wd.at[pl.ds(wo0 + n * rows_o, rows_o), :], sem_wo)

    def gu_copy(e, i):
        src, dst = ((wg_hbm, wg), (wu_hbm, wu))[i]
        sl = pl.ds(pl.multiple_of(zs[e] * block, block), block)
        return pltpu.make_async_copy(src.at[sl, :], dst.at[sl, :], sem_gu.at[e, i])

    order = (3, 2, 1, 0)

    def dn_copy(slot):
        e, i = order[slot // tiles], slot % tiles
        return pltpu.make_async_copy(wd_hbm.at[:, aligned(zs[e] * block + i * TILE, TILE)], wd.at[pl.ds(slot * ff, ff), :], sem_dn.at[slot])

    k_copy = pltpu.make_async_copy(k_hbm, wd.at[pl.ds(kv0, batch * cols), pl.ds(0, head)], sem_kv.at[0])
    v_copy = pltpu.make_async_copy(v_hbm, wd.at[pl.ds(kv0, batch * cols), pl.ds(head, head)], sem_kv.at[1])

    for c in small:
        c.start()
    for n in range(q_loc):
        qkv_copy(n).start(priority=1)
    k_copy.start(priority=1)
    v_copy.start(priority=1)
    for n in range(n_dn):
        wo_copy(n).start(priority=1)
    for e in range(n_tp):
        for i in range(2):
            gu_copy(e, i).start(priority=1)

    barrier = pltpu.get_barrier_semaphore()
    greet = [(e, lo, cc) for e in range(n_tp) for lo in range(2) for cc in range(2)][1:]
    for g in greet:
        pl.semaphore_signal(barrier, inc=1, device_id=device(*g), device_id_type=MESH)

    phase("x_wait")
    for c in small:
        c.wait()
    phase("norm")
    xv = xb[...].astype(F32)
    inv = lax.rsqrt(jnp.mean(xv * xv, axis=-1, keepdims=True) + EPS)
    nrm[...] = (xv * inv * ga[...].reshape(1, width).astype(F32)).astype(BF)
    for r in range(2):
        xf[r] = xv[r * half:(r + 1) * half]
    gain = gm[...].reshape(1, width).astype(F32)
    for e in range(n_tp):
        gmx[e] = gain[:, e * block:(e + 1) * block]

    rows_i = lax.broadcasted_iota(jnp.int32, (batch, head), 0)
    lane = lax.broadcasted_iota(jnp.int32, (batch, head), 1)
    pos = jnp.zeros((batch, head), F32)
    for b in range(batch):
        pos = jnp.where(rows_i == b, ctx_ref[b].astype(F32), pos)
    angle = pos * freq[0:1, :]
    cos_t = jnp.cos(angle)
    sin_t = jnp.sin(angle)
    sin_t = jnp.where(lane < head // 2, -sin_t, sin_t)

    phase("barrier")
    pl.semaphore_wait(barrier, len(greet))
    phase("qkv")
    q_sends = []
    for n in range(q_loc):
        qkv_copy(n).wait()
        mid = width // 2
        lo_half = jnp.dot(nrm[:, :mid], wd[n * width:n * width + mid, :], preferred_element_type=F32)
        hi_half = jnp.dot(nrm[:, mid:], wd[n * width + mid:(n + 1) * width, :], preferred_element_type=F32)
        slot = core * q_loc + n
        qkv[slot] = lo_half + hi_half
        c = remote(qkv.at[slot], qkv.at[slot], s_q.at[n], r_q.at[n], device(0, 0, 1))
        c.start()
        q_sends.append(c)
    phase("qkv_swap")
    for c in q_sends:
        c.wait_recv()
    phase("rope")

    def column(j):
        return qkv[j // 2, :, (j % 2) * head:(j % 2 + 1) * head]

    def rotary(v):
        return (v * cos_t + pltpu.roll(v, head // 2, 1) * sin_t).astype(BF).astype(F32)

    for g in range(kv_loc):
        base = g * (group + 2)
        for r in range(group):
            qs[pl.ds(g * group + r, batch, stride=heads), :] = rotary(column(base + r))
        key = rotary(column(base + group))
        val = column(base + group + 1).astype(BF).astype(F32)
        new_ref[g] = key
        new_ref[kv_loc + g] = val
        for r in range(group):
            kn[pl.ds(g * group + r, batch, stride=heads), :] = key
            vn[pl.ds(g * group + r, batch, stride=heads), :] = val

    phase("kv_wait")
    k_copy.wait()
    v_copy.wait()
    phase("scores")
    scale = head ** -0.5
    for b in range(batch):
        q_b = qs[b * heads:(b + 1) * heads, :].astype(BF)
        k_b = wd[kv0 + b * cols:kv0 + (b + 1) * cols, 0:head]
        sc[b] = lax.dot_general(q_b, k_b, (((1,), (1,)), ((), ())), preferred_element_type=F32)
    phase("softmax")
    s_new = jnp.sum(qs[...] * kn[...], axis=-1, keepdims=True) * scale
    col_i = lax.broadcasted_iota(jnp.int32, (heads, cols), 1)
    row_i = lax.broadcasted_iota(jnp.int32, (heads, cols), 0)
    own = (col_i % kv_loc) == (row_i // group)
    t_i = col_i // kv_loc
    lane_h = lax.broadcasted_iota(jnp.int32, (heads, head), 1)
    p_new = []
    for b in range(batch):
        here = ctx_ref[b] - kvp * block_len
        fresh = s_new[b * heads:(b + 1) * heads]
        is_new = own & (t_i == here)
        s = jnp.where(is_new, fresh, sc[b] * scale)
        s = jnp.where(own & (t_i <= here), s, NEG_FILL)
        m = jnp.max(s, axis=-1, keepdims=True)
        p = jnp.exp(s - m)
        total = jnp.sum(p, axis=-1, keepdims=True)
        p_new.append(jnp.max(jnp.where(is_new, p, 0.0), axis=-1, keepdims=True).astype(BF).astype(F32))
        pr[b] = jnp.where(is_new, 0.0, p).astype(BF)
        mlx[pl.ds(b, heads, stride=batch), :] = jnp.where(lane_h < head // 2, m, total)
    phase("values")
    for b in range(batch):
        v_b = wd[kv0 + b * cols:kv0 + (b + 1) * cols, head:2 * head]
        o = jnp.dot(pr[b], v_b, preferred_element_type=F32)
        accx[pl.ds(b, heads, stride=batch), :] = o + p_new[b] * vn[b * heads:(b + 1) * heads, :]

    phase("exchange")
    rows = heads // n_kvp * batch
    sent = []
    for d, (lo, cc) in enumerate(((1, 1), (1, 0), (0, 1))):
        to = ys[lo] * 2 + cores[cc]
        for i, (src, dst) in enumerate(((accx, racc), (mlx, rml))):
            c = remote(src.at[pl.ds(pl.multiple_of(to * rows, rows), rows), :], dst.at[kvp], s_x.at[2 * d + i], r_x.at[2 * d + i], device(0, lo, cc))
            c.start()
            sent.append(c)
    early = [n for n in range(n_dn) if (n + 1) * ff <= wo0]
    for n in early:
        dn_copy(n).start(priority=1)
    mine = pl.ds(pl.multiple_of(kvp * rows, rows), rows)
    racc[kvp] = accx[mine, :]
    rml[kvp] = mlx[mine, :]
    for c in sent:
        c.wait()
    for c in q_sends:
        c.wait_send()
    phase("combine")
    ml = [rml[i] for i in range(n_kvp)]
    top = functools.reduce(jnp.maximum, ml)
    wt = [jnp.exp(v[:, 0:1] - top[:, 0:1]) for v in ml]
    den = sum(a * v[:, head // 2:head // 2 + 1] for a, v in zip(wt, ml))
    num = sum(a * racc[i] for i, a in enumerate(wt))
    a_f = num / den
    a_own = jnp.concatenate([a_f[r * batch:(r + 1) * batch] for r in range(rows // batch)], axis=1).astype(BF)

    def span(chip):
        return aligned(chip * piece, piece)

    def scatter_sum(step, tile):
        a, b = {}, {}

        def pass_on(e):
            a[e].wait_recv()
            sl = aligned(zs[e] * block, block)
            part[core, :, sl] = part[core, :, sl] + recv_a[step, e]
            for lo in (1, 0):
                i = 2 * e + lo - 1
                if i >= 0:
                    b[i] = remote(part.at[core, :, span(zs[e] * 2 + ys[lo])], recv_b.at[step, i], s_b.at[step, i], r_b.at[step, i], device(e, lo))
                    b[i].start()

        before = None
        for k, e in enumerate(order):
            tile(k, e)
            sl = aligned(zs[e] * block, block)
            a[e] = remote(part.at[1 - core, :, sl], recv_a.at[step, e], s_a.at[step, e], r_a.at[step, e], device(0, 0, 1))
            a[e].start()
            if before is not None:
                pass_on(before)
            before = e
        pass_on(before)
        phase("scatter")
        total = part[core, :, span(me)]
        for i in reversed(range(chips - 1)):
            b[i].wait_recv()
            total = total + recv_b[step, i]
        return total, list(a.values()) + list(b.values())

    def store_tile(e, i, r):
        sl = aligned(zs[e] * block + i * TILE, TILE)
        part[0, :, sl] = r[:half]
        part[1, :, sl] = r[half:]

    class Gather:
        def __init__(self, step, near_first):
            self.step = step
            self.out, self.fwd = {}, {}
            view = full.at[step, core, :, span(me)]
            todo = [(e, lo) for e in range(n_tp) for lo in (0, 1)][1:]
            for e, lo in todo if near_first else todo[::-1]:
                i = 2 * e + lo - 1
                self.out[e, lo] = remote(view, view, s_c.at[step, i], r_c.at[step, i], device(e, lo))
                self.out[e, lo].start()
            self.forward(0, 0)

        def forward(self, e, lo):
            view = full.at[self.step, core, :, span(zs[e] * 2 + ys[lo])]
            i = 2 * e + lo
            self.fwd[e, lo] = remote(view, view, s_d.at[self.step, i], r_d.at[self.step, i], device(0, 0, 1))
            self.fwd[e, lo].start()

        def arrive(self, e):
            for lo in (0, 1):
                if (e, lo) != (0, 0):
                    self.out[e, lo].wait_recv()
                    self.forward(e, lo)

        def settle(self, e):
            for lo in (0, 1):
                self.fwd[e, lo].wait_recv()

        def copies(self):
            return list(self.out.values()) + list(self.fwd.values())

    phase("wo")
    for n in range(n_dn):
        wo_copy(n).wait()

    def wo_tile(k, e):
        for i in range(tiles):
            at = pl.multiple_of(wo0 + (zs[e] * tiles + i) * rows_o, rows_o)
            store_tile(e, i, jnp.dot(a_own, wd[pl.ds(at, rows_o), :], preferred_element_type=F32))

    total, moving = scatter_sum(0, wo_tile)
    for n in range(n_dn):
        if n not in early:
            dn_copy(n).start(priority=1)
    h_own = (xf[core, :, span(me)] + total).astype(BF).astype(F32)
    full[0, core, :, span(me)] = h_own
    lane_p = lax.broadcasted_iota(jnp.int32, (half, LANES), 1)
    row_p = lax.broadcasted_iota(jnp.int32, (half, LANES), 0)
    squares = jnp.sum(h_own * h_own, axis=-1, keepdims=True)
    ss_id = me * 2 + core
    ssb[ss_id] = jnp.sum(jnp.where(lane_p == row_p, squares, 0.0), axis=0, keepdims=True)
    for i, g in enumerate(greet):
        c = remote(ssb.at[ss_id], ssb.at[ss_id], s_s.at[i], r_s.at[i], device(*g))
        c.start()
        moving.append(c)
    ss_copies = moving[-len(greet):]
    gather = Gather(0, True)
    moving += gather.copies()[:0]

    phase("gather_near")
    gather.arrive(0)
    gather.arrive(1)
    phase("squares")
    for c in ss_copies:
        c.wait_recv()
    sums = [sum(ssb[2 * q + c] for q in range(chips)) for c in range(2)]
    both = jnp.where(rows_i < half, sums[0], sums[1])
    mean = jnp.sum(jnp.where(lane == rows_i % half, both, 0.0), axis=-1, keepdims=True) / width
    inv2 = lax.rsqrt(mean + EPS)

    def gate_up(e):
        phase(f"gu_wait{e}")
        gather.settle(e)
        for i in range(2):
            gu_copy(e, i).wait()
        phase(f"gate_up{e}")
        sl = aligned(zs[e] * block, block)
        hv = jnp.concatenate([full[0, 0, :, sl], full[0, 1, :, sl]], axis=0)
        nv = (hv * inv2 * gmx[zs[e]]).astype(BF)
        wr = pl.ds(pl.multiple_of(zs[e] * block, block), block)
        for j in range(n_gu):
            g_v = jnp.dot(nv, wg[wr, j * TILE:(j + 1) * TILE], preferred_element_type=F32)
            u_v = jnp.dot(nv, wu[wr, j * TILE:(j + 1) * TILE], preferred_element_type=F32)
            if e > 0:
                g_v = acc_g[j] + g_v
                u_v = acc_u[j] + u_v
            if e < n_tp - 1:
                acc_g[j] = g_v
                acc_u[j] = u_v
            else:
                act[:, j * TILE:(j + 1) * TILE] = (jax.nn.silu(g_v) * u_v).astype(BF)

    gate_up(0)
    for e in range(1, n_tp):
        if e + 1 < n_tp:
            phase("gather")
            gather.arrive(e + 1)
        gate_up(e)
    for c in moving + gather.copies():
        c.wait_send()

    def dn_tile(k, e):
        phase(f"dn_wait{k}")
        for i in range(tiles):
            dn_copy(k * tiles + i).wait()
        phase(f"down{k}")
        for i in range(tiles):
            at = (k * tiles + i) * ff
            lo_half = jnp.dot(act[:, :ff // 2], wd[at:at + ff // 2, :], preferred_element_type=F32)
            hi_half = jnp.dot(act[:, ff // 2:], wd[at + ff // 2:at + ff, :], preferred_element_type=F32)
            store_tile(e, i, lo_half + hi_half)
        phase(f"pass{k}")

    total, moving = scatter_sum(1, dn_tile)
    full[1, core, :, span(me)] = (full[0, core, :, span(me)] + total).astype(BF).astype(F32)
    phase("gather2")
    last = Gather(1, False)
    for e in range(n_tp):
        last.arrive(e)
    phase("gather_core")
    for e in range(n_tp):
        last.settle(e)
    phase("output")
    out_ref[...] = jnp.concatenate([full[1, 0], full[1, 1]], axis=0).astype(BF)
    phase("drain")
    for c in moving + last.copies():
        c.wait_send()
    phase(None)


def _cache_kernel(dims, ctx_hbm, new_hbm, x_hbm, k_hbm, v_hbm, xo_hbm, ko_hbm, vo_hbm, ctx_ref, new_ref, xb, kbuf, vbuf, sem_s, sem_i, sem_o):
    batch, block_len, kv_loc, chunks = dims
    kvp = lax.axis_index("kvp")
    size = batch // chunks
    jobs = [(i, c) for c in range(chunks) for i in range(2)]

    def load(i, c):
        src, buf = ((k_hbm, kbuf), (v_hbm, vbuf))[i]
        sl = pl.ds(c * size, size)
        return pltpu.make_async_copy(src.at[sl], buf.at[sl], sem_i.at[i, c])

    def save(i, c):
        dst, buf = ((ko_hbm, kbuf), (vo_hbm, vbuf))[i]
        sl = pl.ds(c * size, size)
        return pltpu.make_async_copy(buf.at[sl], dst.at[sl], sem_o.at[i, c])

    small = [pltpu.make_async_copy(s, d, sem_s.at[i]) for i, (s, d) in enumerate(((ctx_hbm, ctx_ref), (new_hbm, new_ref), (x_hbm, xb)))]
    for c in small:
        c.start()
    for j in jobs:
        load(*j).start(priority=1)
    for c in small:
        c.wait()
    x_save = pltpu.make_async_copy(xb, xo_hbm, sem_s.at[3])
    x_save.start()
    for i, c in jobs:
        load(i, c).wait()
        buf = (kbuf, vbuf)[i]
        for b in range(c * size, (c + 1) * size):
            here = ctx_ref[b] - kvp * block_len

            @pl.when((here >= 0) & (here < block_len))
            def _():
                rows = [new_ref[i * kv_loc + g, b:b + 1, :] for g in range(kv_loc)]
                buf[b, jnp.clip(here, 0, block_len - 1)] = jnp.concatenate(rows, axis=0).astype(BF)

        save(i, c).start(priority=1)
    x_save.wait()
    for j in jobs:
        save(*j).wait()


def solution(mesh):
    n_tp, n_kvp = mesh.shape["tp"], mesh.shape["kvp"]
    x_spec = P("dp", None)
    cache_spec = P("dp", "kvp", "tp", None)
    model_axes = ("tp", "kvp")

    def layer_step(x_in, ctx_len, g_attn, g_mlp, w_qkv, w_o, w_gate, w_up, w_down, k_cache, v_cache):
        batch, block_len, kv_loc, head = k_cache.shape
        width = x_in.shape[1]
        ff = w_gate.shape[1]
        group = w_qkv.shape[1] // (kv_loc * head) - 2
        heads = kv_loc * group
        chips = n_tp * n_kvp // 2
        n_qkv, n_gu, n_dn = w_qkv.shape[1] // TILE, ff // TILE, width // TILE
        half = batch // 2
        rows = heads // n_kvp * batch
        freq = (ROPE_THETA ** (-2.0 * np.arange(head // 2) / head)).astype(np.float32)
        freq = jnp.asarray(np.tile(np.concatenate([freq, freq])[None], (8, 1)))
        flat = (batch * block_len * kv_loc, head)
        hbm = pl.BlockSpec(memory_space=pl.ANY)
        vmem = pl.BlockSpec(memory_space=pltpu.VMEM)
        dma = pltpu.SemaphoreType.DMA
        peers = chips - 1
        dims = (batch, width, ff, kv_loc, group, head, block_len, n_tp, n_kvp)
        x_out, new = pl.pallas_call(
            functools.partial(_layer_kernel, dims),
            out_shape=(jax.ShapeDtypeStruct((batch, width), BF), jax.ShapeDtypeStruct((2 * kv_loc, batch, head), F32)),
            in_specs=[hbm] * 12,
            out_specs=(vmem, vmem),
            scratch_shapes=[
                pltpu.SMEM((batch,), jnp.int32),
                pltpu.VMEM((width, ff), BF),
                pltpu.VMEM((width, ff), BF),
                pltpu.VMEM((ff * width // TILE, TILE), BF),
                pltpu.VMEM((batch, width), BF),
                pltpu.VMEM((width,), BF),
                pltpu.VMEM((width,), BF),
                pltpu.VMEM((8, head), F32),
                pltpu.VMEM((2, half, width), F32),
                pltpu.VMEM((batch, width), BF),
                pltpu.VMEM((n_tp, 1, width // n_tp), F32),
                pltpu.VMEM((n_qkv, batch, TILE), F32),
                pltpu.VMEM((batch * heads, head), F32),
                pltpu.VMEM((batch * heads, head), F32),
                pltpu.VMEM((batch * heads, head), F32),
                pltpu.VMEM((batch, heads, kv_loc * block_len), F32),
                pltpu.VMEM((batch, heads, kv_loc * block_len), BF),
                pltpu.VMEM((batch * heads, head), F32),
                pltpu.VMEM((batch * heads, head), F32),
                pltpu.VMEM((n_kvp, rows, head), F32),
                pltpu.VMEM((n_kvp, rows, head), F32),
                pltpu.VMEM((2, half, width), F32),
                pltpu.VMEM((2, n_tp, half, width // n_tp), F32),
                pltpu.VMEM((2, peers, half, width // chips), F32),
                pltpu.VMEM((2, 2, half, width), F32),
                pltpu.VMEM((n_tp * n_kvp, 1, LANES), F32),
                pltpu.VMEM((n_gu, batch, TILE), F32),
                pltpu.VMEM((n_gu, batch, TILE), F32),
                pltpu.VMEM((batch, ff), BF),
                dma((5,)), dma((n_qkv // 2,)), dma((2,)), dma, dma((n_tp, 2)), dma((n_dn,)),
                dma((n_qkv // 2,)), dma((n_qkv // 2,)), dma((6,)), dma((6,)), dma((n_tp * n_kvp - 1,)), dma((n_tp * n_kvp - 1,)),
                dma((2, n_tp)), dma((2, n_tp)), dma((2, peers)), dma((2, peers)), dma((2, peers)), dma((2, peers)),
                dma((2, peers + 1)), dma((2, peers + 1)),
            ],
            compiler_params=pltpu.CompilerParams(collective_id=0, has_side_effects=True, vmem_limit_bytes=VMEM_BYTES),
            name="layer",
        )(ctx_len, x_in, g_attn, g_mlp, freq, w_qkv, w_o, w_gate, w_up, w_down, k_cache.reshape(flat), v_cache.reshape(flat))
        chunks = 4
        x_out, k_out, v_out = pl.pallas_call(
            functools.partial(_cache_kernel, (batch, block_len, kv_loc, chunks)),
            out_shape=(jax.ShapeDtypeStruct((batch, width), BF), jax.ShapeDtypeStruct(k_cache.shape, BF), jax.ShapeDtypeStruct(v_cache.shape, BF)),
            in_specs=[hbm] * 5,
            out_specs=(hbm, hbm, hbm),
            scratch_shapes=[
                pltpu.SMEM((batch,), jnp.int32), pltpu.VMEM((2 * kv_loc, batch, head), F32), pltpu.VMEM((batch, width), BF),
                pltpu.VMEM(k_cache.shape, BF), pltpu.VMEM(v_cache.shape, BF), dma((4,)), dma((2, chunks)), dma((2, chunks)),
            ],
            compiler_params=pltpu.CompilerParams(vmem_limit_bytes=VMEM_BYTES),
            name="cache",
        )(ctx_len, new, x_out, k_cache, v_cache)
        return x_out, k_out, v_out

    in_specs = (x_spec, P("dp"), P(None), P(None), P(None, "tp"), P(model_axes, None), P(None, model_axes), P(None, model_axes), P(model_axes, None), cache_spec, cache_spec)
    return jax.shard_map(layer_step, mesh=mesh, in_specs=in_specs, out_specs=(x_spec, cache_spec, cache_spec), check_vma=False)
```

```python
import functools

import jax
import jax.numpy as jnp
import numpy as np
from jax import lax
from jax.experimental import pallas as pl
from jax.experimental.pallas import tpu as pltpu
from jax.sharding import PartitionSpec as P

ROPE_THETA = 500000.0
EPS = 1e-5
NEG_FILL = -1e30
MESH = pl.DeviceIdType.MESH
BF = jnp.bfloat16
F32 = jnp.float32
LANES = 128
TILE = 256
VMEM_BYTES = 67_043_328


class _Phase:
    def __init__(self):
        self.scope = None

    def __call__(self, name):
        if self.scope is not None:
            self.scope.__exit__(None, None, None)
        self.scope = None
        if name:
            self.scope = jax.named_scope(name)
            self.scope.__enter__()


def _layer_kernel(dims, ctx_hbm, x_hbm, ga_hbm, gm_hbm, freq_hbm, wqkv_hbm, wo_hbm, wg_hbm, wu_hbm, wd_hbm, k_hbm, v_hbm,
                  out_ref, new_ref,
                  ctx_ref, wg, wu, wd, xb, ga, gm, freq, xf, nrm, gmx, qkv, qkv2, qs, kn, vn, sc, pr, accx, mlx, racc, rml, part, recv_a, recv_b, recv_c, full,
                  ssb, acc_g, acc_u, act,
                  sem_in, sem_qkv, sem_kv, sem_wo, sem_gu, sem_dn, s_q, r_q, s_x, r_x, s_s, r_s, s_a, r_a, s_b, r_b, s_c, r_c, s_gz, r_gz, s_gy, r_gy, s_d, r_d):
    batch, width, ff, kv_loc, group, head, block_len, n_tp, n_kvp = dims
    half = batch // 2
    chips = n_tp * n_kvp // 2
    piece = width // chips
    block = 2 * piece
    tiles = block // TILE
    heads = kv_loc * group
    n_qkv = kv_loc * (group + 2) * head // TILE
    q_loc = n_qkv // 2
    n_gu = ff // TILE
    n_dn = width // TILE
    rows_o = wo_hbm.shape[0]
    cols = kv_loc * block_len
    kv0 = q_loc * width
    wo0 = kv0 + batch * cols
    wo_end = wo0 + n_dn * rows_o

    phase = _Phase()
    phase("loads")
    tp = lax.axis_index("tp")
    kvp = lax.axis_index("kvp")
    core = kvp % 2
    y = kvp // 2
    me = tp * 2 + y
    pal = kvp + 1 - 2 * core
    zs = [tp, tp + 1 - 2 * (tp % 2), (tp + 2) % 4, 3 - tp]
    ys = [y, 1 - y]
    cores = [core, 1 - core]

    def device(e, lo, cc=0):
        return {"tp": zs[e], "kvp": ys[lo] * 2 + cores[cc]}

    def remote(src, dst, send, recv, to):
        return pltpu.make_async_remote_copy(src, dst, send, recv, device_id=to, device_id_type=MESH)

    def aligned(start, size):
        return pl.ds(pl.multiple_of(start, LANES), size)

    small = [pltpu.make_async_copy(s, d, sem_in.at[i]) for i, (s, d) in enumerate(((x_hbm, xb), (ga_hbm, ga), (freq_hbm, freq), (ctx_hbm, ctx_ref), (gm_hbm, gm)))]

    def qkv_copy(n):
        return pltpu.make_async_copy(wqkv_hbm.at[:, aligned((core * q_loc + n) * TILE, TILE)], wd.at[pl.ds(n * width, width), :], sem_qkv.at[n])

    def wo_copy(n):
        return pltpu.make_async_copy(wo_hbm.at[:, pl.ds(n * TILE, TILE)], wd.at[pl.ds(wo0 + n * rows_o, rows_o), :], sem_wo)

    def gu_copy(e, i):
        src, dst = ((wg_hbm, wg), (wu_hbm, wu))[i]
        sl = pl.ds(pl.multiple_of(zs[e] * block, block), block)
        return pltpu.make_async_copy(src.at[sl, :], dst.at[sl, :], sem_gu.at[e, i])

    order = (3, 2, 1, 0)

    def dn_copy(slot):
        e, i = order[slot // tiles], slot % tiles
        return pltpu.make_async_copy(wd_hbm.at[:, aligned(zs[e] * block + i * TILE, TILE)], wd.at[pl.ds(slot * ff, ff), :], sem_dn.at[slot])

    k_copy = pltpu.make_async_copy(k_hbm, wd.at[pl.ds(kv0, batch * cols), pl.ds(0, head)], sem_kv.at[0])
    v_copy = pltpu.make_async_copy(v_hbm, wd.at[pl.ds(kv0, batch * cols), pl.ds(head, head)], sem_kv.at[1])

    for c in small:
        c.start()
    for n in range(q_loc):
        qkv_copy(n).start(priority=1)
    k_copy.start(priority=1)
    v_copy.start(priority=1)
    for n in range(n_dn):
        wo_copy(n).start(priority=1)
    def start_gu(e):
        for i in range(2):
            gu_copy(e, i).start(priority=1)

    barrier = pltpu.get_barrier_semaphore()
    greet = [(e, lo, cc) for e in range(n_tp) for lo in range(2) for cc in range(2)][1:]
    for g in greet:
        pl.semaphore_signal(barrier, inc=1, device_id=device(*g), device_id_type=MESH)

    phase("x_wait")
    for c in small:
        c.wait()
    phase("norm")
    xv = xb[...].astype(F32)
    inv = lax.rsqrt(jnp.mean(xv * xv, axis=-1, keepdims=True) + EPS)
    nrm[...] = (xv * inv * ga[...].reshape(1, width).astype(F32)).astype(BF)
    for r in range(2):
        xf[r] = xv[r * half:(r + 1) * half]
    gain = gm[...].reshape(1, width).astype(F32)
    for e in range(n_tp):
        gmx[e] = gain[:, e * block:(e + 1) * block]

    rows_i = lax.broadcasted_iota(jnp.int32, (batch, head), 0)
    lane = lax.broadcasted_iota(jnp.int32, (batch, head), 1)
    pos = jnp.zeros((batch, head), F32)
    for b in range(batch):
        pos = jnp.where(rows_i == b, ctx_ref[b].astype(F32), pos)
    angle = pos * freq[0:1, :]
    cos_t = jnp.cos(angle)
    sin_t = jnp.sin(angle)
    sin_t = jnp.where(lane < head // 2, -sin_t, sin_t)

    start_gu(0)
    phase("qkv")
    q_sends = []
    for n in range(q_loc):
        qkv_copy(n).wait()
        mid = width // 2
        lo_half = jnp.dot(nrm[:, :mid], wd[n * width:n * width + mid, :], preferred_element_type=F32)
        hi_half = jnp.dot(nrm[:, mid:], wd[n * width + mid:(n + 1) * width, :], preferred_element_type=F32)
        qkv2[0, n] = lo_half
        qkv2[1, n] = hi_half
    start_gu(1)
    phase("barrier")
    pl.semaphore_wait(barrier, len(greet))
    for n in range(q_loc):
        slot = core * q_loc + n
        qkv[slot] = qkv2[0, n] + qkv2[1, n]
        c = remote(qkv.at[slot], qkv.at[slot], s_q.at[n], r_q.at[n], device(0, 0, 1))
        c.start()
        q_sends.append(c)
    phase("qkv_swap")
    for c in q_sends:
        c.wait_recv()
    phase("rope")

    def column(j):
        return qkv[j // 2, :, (j % 2) * head:(j % 2 + 1) * head]

    def rotary(v):
        return (v * cos_t + pltpu.roll(v, head // 2, 1) * sin_t).astype(BF).astype(F32)

    for g in range(kv_loc):
        base = g * (group + 2)
        for r in range(group):
            qs[pl.ds(g * group + r, batch, stride=heads), :] = rotary(column(base + r))
        key = rotary(column(base + group))
        val = column(base + group + 1).astype(BF).astype(F32)
        new_ref[g] = key
        new_ref[kv_loc + g] = val
        for r in range(group):
            kn[pl.ds(g * group + r, batch, stride=heads), :] = key
            vn[pl.ds(g * group + r, batch, stride=heads), :] = val

    phase("kv_wait")
    k_copy.wait()
    v_copy.wait()
    phase("scores")
    scale = head ** -0.5
    for b in range(batch):
        q_b = qs[b * heads:(b + 1) * heads, :].astype(BF)
        k_b = wd[kv0 + b * cols:kv0 + (b + 1) * cols, 0:head]
        sc[b] = lax.dot_general(q_b, k_b, (((1,), (1,)), ((), ())), preferred_element_type=F32)
    phase("softmax")
    s_new = jnp.sum(qs[...] * kn[...], axis=-1, keepdims=True) * scale
    col_i = lax.broadcasted_iota(jnp.int32, (heads, cols), 1)
    row_i = lax.broadcasted_iota(jnp.int32, (heads, cols), 0)
    own = (col_i % kv_loc) == (row_i // group)
    t_i = col_i // kv_loc
    lane_h = lax.broadcasted_iota(jnp.int32, (heads, head), 1)
    p_new = []
    stat = jnp.zeros((heads, head), F32)
    for b in range(batch):
        here = ctx_ref[b] - kvp * block_len
        fresh = s_new[b * heads:(b + 1) * heads]
        is_new = own & (t_i == here)
        s = jnp.where(is_new, fresh, sc[b] * scale)
        s = jnp.where(own & (t_i <= here), s, NEG_FILL)
        m = jnp.max(s, axis=-1, keepdims=True)
        p = jnp.exp(s - m)
        total = jnp.sum(p, axis=-1, keepdims=True)
        p_new.append(jnp.max(jnp.where(is_new, p, 0.0), axis=-1, keepdims=True).astype(BF).astype(F32))
        pr[b] = jnp.where(is_new, 0.0, p).astype(BF)
        stat = jnp.where(lane_h == b, m, jnp.where(lane_h == batch + b, total, stat))
    for h in range(heads):
        mlx[h] = stat[h:h + 1]
    phase("values")
    for b in range(batch):
        v_b = wd[kv0 + b * cols:kv0 + (b + 1) * cols, head:2 * head]
        o = jnp.dot(pr[b], v_b, preferred_element_type=F32)
        accx[pl.ds(b, heads, stride=batch), :] = o + p_new[b] * vn[b * heads:(b + 1) * heads, :]

    phase("exchange")
    heads_o = heads // n_kvp
    rows = heads_o * batch
    sent = []
    for d, (lo, cc) in enumerate(((1, 1), (1, 0), (0, 1))):
        to = ys[lo] * 2 + cores[cc]
        for i, (src, dst) in enumerate(((accx.at[pl.ds(pl.multiple_of(to * rows, rows), rows), :], racc), (mlx.at[pl.ds(to * heads_o, heads_o)], rml))):
            c = remote(src, dst.at[kvp], s_x.at[2 * d + i], r_x.at[2 * d + i], device(0, lo, cc))
            c.start()
            sent.append(c)
    start_gu(2)
    start_gu(3)
    mine = pl.ds(pl.multiple_of(kvp * rows, rows), rows)
    racc[kvp] = accx[mine, :]
    rml[kvp] = mlx[pl.ds(kvp * heads_o, heads_o)]
    for c in sent:
        c.wait()
    for c in q_sends:
        c.wait_send()
    phase("combine")
    early = [n for n in range(n_dn) if (n + 1) * ff <= wo0]
    for n in early:
        dn_copy(n).start(priority=1)

    def spread(row, shift):
        return jnp.sum(jnp.where(lane == rows_i + shift, row, 0.0), axis=-1, keepdims=True)

    parts = []
    for r in range(heads_o):
        m_s = [spread(rml[i, r], 0) for i in range(n_kvp)]
        l_s = [spread(rml[i, r], batch) for i in range(n_kvp)]
        top = functools.reduce(jnp.maximum, m_s)
        wt = [jnp.exp(m - top) for m in m_s]
        den = sum(a * l for a, l in zip(wt, l_s))
        num = sum(a * racc[i, r * batch:(r + 1) * batch] for i, a in enumerate(wt))
        parts.append(num / den)
    a_own = jnp.concatenate(parts, axis=1).astype(BF)

    def span(chip):
        return aligned(chip * piece, piece)

    def scatter_sum(step, tile):
        a, b, c = {}, {}, {}

        def to_y(e):
            phase(f"core{e}")
            a[e].wait_recv()
            sl = aligned(zs[e] * block, block)
            part[core, :, sl] = part[core, :, sl] + recv_a[step, e]
            b[e] = remote(part.at[core, :, span(zs[e] * 2 + 1 - y)], recv_b.at[step, e], s_b.at[step, e], r_b.at[step, e], device(0, 1))
            b[e].start()

        def to_z(e):
            phase(f"y{e}")
            b[e].wait_recv()
            sl = span(zs[e] * 2 + y)
            part[core, :, sl] = part[core, :, sl] + recv_b[step, e]
            if e > 0:
                c[e] = remote(part.at[core, :, sl], recv_c.at[step, e - 1], s_c.at[step, e - 1], r_c.at[step, e - 1], device(e, 0))
                c[e].start()

        for k in range(n_tp + 2):
            if k < n_tp:
                e = order[k]
                tile(k, e)
                sl = aligned(zs[e] * block, block)
                a[e] = remote(part.at[1 - core, :, sl], recv_a.at[step, e], s_a.at[step, e], r_a.at[step, e], device(0, 0, 1))
                a[e].start()
            if 0 <= k - 1 < n_tp:
                to_y(order[k - 1])
            if 0 <= k - 2 < n_tp:
                to_z(order[k - 2])
        phase("z")
        total = part[core, :, span(me)]
        for e in order[:-1]:
            c[e].wait_recv()
            total = total + recv_c[step, e - 1]
        return total, [*a.values(), *b.values(), *c.values()]

    def store_tile(e, i, r):
        sl = aligned(zs[e] * block + i * TILE, TILE)
        part[0, :, sl] = r[:half]
        part[1, :, sl] = r[half:]

    class Gather:
        def __init__(self, step):
            self.step = step
            self.zc, self.yc, self.fwd = {}, {}, {}
            for e in (1, 2, 3):
                self.zc[e] = self.copy(0, y, s_gz, r_gz, e - 1, device(e, 0))
            self.along_y(0)
            self.across(0, 0)

        def copy(self, e, yy, send, recv, i, to):
            view = full.at[self.step, core, :, span(zs[e] * 2 + yy)]
            c = remote(view, view, send.at[self.step, i], recv.at[self.step, i], to)
            c.start()
            return c

        def along_y(self, e):
            self.yc[e] = self.copy(e, y, s_gy, r_gy, e, device(0, 1))

        def across(self, e, lo):
            self.fwd[e, lo] = self.copy(e, ys[lo], s_d, r_d, 2 * e + lo, device(0, 0, 1))

        def from_z(self, e):
            self.zc[e].wait_recv()
            self.along_y(e)
            self.across(e, 0)

        def from_y(self, e):
            self.yc[e].wait_recv()
            self.across(e, 1)

        def settle(self, e):
            for lo in (0, 1):
                self.fwd[e, lo].wait_recv()

        def copies(self):
            return [*self.zc.values(), *self.yc.values(), *self.fwd.values()]

    phase("wo")
    for n in range(n_dn):
        wo_copy(n).wait()

    def wo_tile(k, e):
        for i in range(tiles):
            at = pl.multiple_of(wo0 + (zs[e] * tiles + i) * rows_o, rows_o)
            store_tile(e, i, jnp.dot(a_own, wd[pl.ds(at, rows_o), :], preferred_element_type=F32))

    total, moving = scatter_sum(0, wo_tile)
    for n in range(n_dn):
        if n not in early:
            dn_copy(n).start(priority=1)
    h_own = (xf[core, :, span(me)] + total).astype(BF).astype(F32)
    full[0, core, :, span(me)] = h_own
    lane_p = lax.broadcasted_iota(jnp.int32, (half, LANES), 1)
    row_p = lax.broadcasted_iota(jnp.int32, (half, LANES), 0)
    squares = jnp.sum(h_own * h_own, axis=-1, keepdims=True)
    ss_id = me * 2 + core
    ssb[ss_id] = jnp.sum(jnp.where(lane_p == row_p, squares, 0.0), axis=0, keepdims=True)
    for i, g in enumerate(greet):
        c = remote(ssb.at[ss_id], ssb.at[ss_id], s_s.at[i], r_s.at[i], device(*g))
        c.start()
        moving.append(c)
    ss_copies = moving[-len(greet):]
    gather = Gather(0)

    phase("gather_near")
    gather.from_y(0)
    gather.from_z(1)
    phase("squares")
    for c in ss_copies:
        c.wait_recv()
    sums = [sum(ssb[2 * q + c] for q in range(chips)) for c in range(2)]
    both = jnp.where(rows_i < half, sums[0], sums[1])
    mean = jnp.sum(jnp.where(lane == rows_i % half, both, 0.0), axis=-1, keepdims=True) / width
    inv2 = lax.rsqrt(mean + EPS)

    def gate_up(e):
        phase(f"gu_wait{e}")
        gather.settle(e)
        for i in range(2):
            gu_copy(e, i).wait()
        phase(f"gate_up{e}")
        sl = aligned(zs[e] * block, block)
        hv = jnp.concatenate([full[0, 0, :, sl], full[0, 1, :, sl]], axis=0)
        nv = (hv * inv2 * gmx[zs[e]]).astype(BF)
        wr = pl.ds(pl.multiple_of(zs[e] * block, block), block)
        for j in range(n_gu):
            g_v = jnp.dot(nv, wg[wr, j * TILE:(j + 1) * TILE], preferred_element_type=F32)
            u_v = jnp.dot(nv, wu[wr, j * TILE:(j + 1) * TILE], preferred_element_type=F32)
            if e > 0:
                g_v = acc_g[j] + g_v
                u_v = acc_u[j] + u_v
            if e < n_tp - 1:
                acc_g[j] = g_v
                acc_u[j] = u_v
            else:
                act[:, j * TILE:(j + 1) * TILE] = (jax.nn.silu(g_v) * u_v).astype(BF)

    phase("gather_z")
    gather.from_z(2)
    gather.from_z(3)
    gate_up(0)
    phase("gather_y1")
    gather.from_y(1)
    gate_up(1)
    phase("gather_y2")
    gather.from_y(2)
    gather.from_y(3)
    gate_up(2)
    gate_up(3)
    for c in moving + gather.copies():
        c.wait_send()

    def dn_tile(k, e):
        phase(f"dn_wait{k}")
        for i in range(tiles):
            dn_copy(k * tiles + i).wait()
        phase(f"down{k}")
        for i in range(tiles):
            at = (k * tiles + i) * ff
            store_tile(e, i, jnp.dot(act[...], wd[at:at + ff, :], preferred_element_type=F32))

    total, moving = scatter_sum(1, dn_tile)
    full[1, core, :, span(me)] = (full[0, core, :, span(me)] + total).astype(BF).astype(F32)
    phase("gather2")
    last = Gather(1)
    for e in (1, 2, 3):
        last.from_z(e)
    phase("gather2_y")
    for e in range(n_tp):
        last.from_y(e)
    phase("gather_core")
    for e in range(n_tp):
        last.settle(e)
    phase("output")
    out_ref[...] = jnp.concatenate([full[1, 0], full[1, 1]], axis=0).astype(BF)
    phase("drain")
    for c in moving + last.copies():
        c.wait_send()
    phase(None)


def _cache_kernel(dims, ctx_hbm, new_hbm, x_hbm, k_hbm, v_hbm, xo_hbm, ko_hbm, vo_hbm, ctx_ref, new_ref, xb, kbuf, vbuf, sem_s, sem_i, sem_o):
    batch, block_len, kv_loc, chunks = dims
    kvp = lax.axis_index("kvp")
    size = batch // chunks
    jobs = [(i, c) for c in range(chunks) for i in range(2)]

    def load(i, c):
        src, buf = ((k_hbm, kbuf), (v_hbm, vbuf))[i]
        sl = pl.ds(c * size, size)
        return pltpu.make_async_copy(src.at[sl], buf.at[sl], sem_i.at[i, c])

    def save(i, c):
        dst, buf = ((ko_hbm, kbuf), (vo_hbm, vbuf))[i]
        sl = pl.ds(c * size, size)
        return pltpu.make_async_copy(buf.at[sl], dst.at[sl], sem_o.at[i, c])

    small = [pltpu.make_async_copy(s, d, sem_s.at[i]) for i, (s, d) in enumerate(((ctx_hbm, ctx_ref), (new_hbm, new_ref), (x_hbm, xb)))]
    for c in small:
        c.start()
    for j in jobs:
        load(*j).start(priority=1)
    for c in small:
        c.wait()
    x_save = pltpu.make_async_copy(xb, xo_hbm, sem_s.at[3])
    x_save.start()
    for i, c in jobs:
        load(i, c).wait()
        buf = (kbuf, vbuf)[i]
        for b in range(c * size, (c + 1) * size):
            here = ctx_ref[b] - kvp * block_len

            @pl.when((here >= 0) & (here < block_len))
            def _():
                rows = [new_ref[i * kv_loc + g, b:b + 1, :] for g in range(kv_loc)]
                buf[b, jnp.clip(here, 0, block_len - 1)] = jnp.concatenate(rows, axis=0).astype(BF)

        save(i, c).start(priority=1)
    x_save.wait()
    for j in jobs:
        save(*j).wait()


def solution(mesh):
    n_tp, n_kvp = mesh.shape["tp"], mesh.shape["kvp"]
    x_spec = P("dp", None)
    cache_spec = P("dp", "kvp", "tp", None)
    model_axes = ("tp", "kvp")

    def layer_step(x_in, ctx_len, g_attn, g_mlp, w_qkv, w_o, w_gate, w_up, w_down, k_cache, v_cache):
        batch, block_len, kv_loc, head = k_cache.shape
        width = x_in.shape[1]
        ff = w_gate.shape[1]
        group = w_qkv.shape[1] // (kv_loc * head) - 2
        heads = kv_loc * group
        chips = n_tp * n_kvp // 2
        n_qkv, n_gu, n_dn = w_qkv.shape[1] // TILE, ff // TILE, width // TILE
        half = batch // 2
        rows = heads // n_kvp * batch
        freq = (ROPE_THETA ** (-2.0 * np.arange(head // 2) / head)).astype(np.float32)
        freq = jnp.asarray(np.tile(np.concatenate([freq, freq])[None], (8, 1)))
        flat = (batch * block_len * kv_loc, head)
        hbm = pl.BlockSpec(memory_space=pl.ANY)
        vmem = pl.BlockSpec(memory_space=pltpu.VMEM)
        dma = pltpu.SemaphoreType.DMA
        dims = (batch, width, ff, kv_loc, group, head, block_len, n_tp, n_kvp)
        x_out, new = pl.pallas_call(
            functools.partial(_layer_kernel, dims),
            out_shape=(jax.ShapeDtypeStruct((batch, width), BF), jax.ShapeDtypeStruct((2 * kv_loc, batch, head), F32)),
            in_specs=[hbm] * 12,
            out_specs=(vmem, vmem),
            scratch_shapes=[
                pltpu.SMEM((batch,), jnp.int32),
                pltpu.VMEM((width, ff), BF),
                pltpu.VMEM((width, ff), BF),
                pltpu.VMEM((ff * width // TILE, TILE), BF),
                pltpu.VMEM((batch, width), BF),
                pltpu.VMEM((width,), BF),
                pltpu.VMEM((width,), BF),
                pltpu.VMEM((8, head), F32),
                pltpu.VMEM((2, half, width), F32),
                pltpu.VMEM((batch, width), BF),
                pltpu.VMEM((n_tp, 1, width // n_tp), F32),
                pltpu.VMEM((n_qkv, batch, TILE), F32),
                pltpu.VMEM((2, n_qkv // 2, batch, TILE), F32),
                pltpu.VMEM((batch * heads, head), F32),
                pltpu.VMEM((batch * heads, head), F32),
                pltpu.VMEM((batch * heads, head), F32),
                pltpu.VMEM((batch, heads, kv_loc * block_len), F32),
                pltpu.VMEM((batch, heads, kv_loc * block_len), BF),
                pltpu.VMEM((batch * heads, head), F32),
                pltpu.VMEM((heads, 1, head), F32),
                pltpu.VMEM((n_kvp, rows, head), F32),
                pltpu.VMEM((n_kvp, heads // n_kvp, 1, head), F32),
                pltpu.VMEM((2, half, width), F32),
                pltpu.VMEM((2, n_tp, half, width // n_tp), F32),
                pltpu.VMEM((2, n_tp, half, width // chips), F32),
                pltpu.VMEM((2, n_tp - 1, half, width // chips), F32),
                pltpu.VMEM((2, 2, half, width), F32),
                pltpu.VMEM((n_tp * n_kvp, 1, LANES), F32),
                pltpu.VMEM((n_gu, batch, TILE), F32),
                pltpu.VMEM((n_gu, batch, TILE), F32),
                pltpu.VMEM((batch, ff), BF),
                dma((5,)), dma((n_qkv // 2,)), dma((2,)), dma, dma((n_tp, 2)), dma((n_dn,)),
                dma((n_qkv // 2,)), dma((n_qkv // 2,)), dma((6,)), dma((6,)), dma((n_tp * n_kvp - 1,)), dma((n_tp * n_kvp - 1,)),
                dma((2, n_tp)), dma((2, n_tp)), dma((2, n_tp)), dma((2, n_tp)), dma((2, n_tp - 1)), dma((2, n_tp - 1)),
                dma((2, n_tp - 1)), dma((2, n_tp - 1)), dma((2, n_tp)), dma((2, n_tp)), dma((2, chips)), dma((2, chips)),
            ],
            compiler_params=pltpu.CompilerParams(collective_id=0, has_side_effects=True, vmem_limit_bytes=VMEM_BYTES),
            name="layer",
        )(ctx_len, x_in, g_attn, g_mlp, freq, w_qkv, w_o, w_gate, w_up, w_down, k_cache.reshape(flat), v_cache.reshape(flat))
        chunks = 4
        x_out, k_out, v_out = pl.pallas_call(
            functools.partial(_cache_kernel, (batch, block_len, kv_loc, chunks)),
            out_shape=(jax.ShapeDtypeStruct((batch, width), BF), jax.ShapeDtypeStruct(k_cache.shape, BF), jax.ShapeDtypeStruct(v_cache.shape, BF)),
            in_specs=[hbm] * 5,
            out_specs=(hbm, hbm, hbm),
            scratch_shapes=[
                pltpu.SMEM((batch,), jnp.int32), pltpu.VMEM((2 * kv_loc, batch, head), F32), pltpu.VMEM((batch, width), BF),
                pltpu.VMEM(k_cache.shape, BF), pltpu.VMEM(v_cache.shape, BF), dma((4,)), dma((2, chunks)), dma((2, chunks)),
            ],
            compiler_params=pltpu.CompilerParams(vmem_limit_bytes=VMEM_BYTES),
            name="cache",
        )(ctx_len, new, x_out, k_cache, v_cache)
        return x_out, k_out, v_out

    in_specs = (x_spec, P("dp"), P(None), P(None), P(None, "tp"), P(model_axes, None), P(None, model_axes), P(None, model_axes), P(model_axes, None), cache_spec, cache_spec)
    return jax.shard_map(layer_step, mesh=mesh, in_specs=in_specs, out_specs=(x_spec, cache_spec, cache_spec), check_vma=False)
```
